32 devices in a mesh: row: 4 (over z), col: 8 (over y, x, core).
Axes of the slice: x: 2, y: 2, z: 4, core: 2. Of those that a mesh axis runs over, the one named last changes fastest.
Arguments:
- a_matrix: bfloat16 [8192, 8192], P('row', 'col'), may hold values from -6 to 6
- a_flags: int32 [64, 64], P('row', 'col'), may hold values from 0 to 1, as said below
- b_matrix: bfloat16 [8192, 16384], P('row', 'col'), may hold values from -0.1875 to 0.1875
- b_flags: int32 [64, 128], P('row', 'col'), may hold values from 0 to 1, as said below
- sections: int32 [2], replicated, may hold values from 0 to 7
Outputs:
- packed: bfloat16 [8192, 16384], P('row', 'col')
- tile_place: int32 [64, 128], P('row', 'col')
The draws below stay inside these ranges and needn't reach their ends.
Inputs may be any that keep to these rules, and one draw needn't show every extreme that they name: `a_flags`: 0 or 1; the 16 x 8 tiles of one device hold at most 64 ones, and some device holds exactly 64. `b_flags`: 0 or 1; each aligned block of 8 x 16 tiles holds at most 64 ones, and some block exactly 64.
All inputs are finite; a program needn't handle non-finite values.
Results may differ from the reference program's by a relative error of at most 0.001.
Values may be sent and summed in bfloat16 or wider, within the bound.
No kernel may reach another device: no remote copies, remote signals or barrier semaphores. Data moves between devices by JAX's collectives and lax.ppermute only.
A program may use at most 128 MiB of HBM per device.

```python
import jax
import jax.numpy as jnp
from jax import lax

TILE = 128
TM_DEV = 16
TN_DEV = 16
KT = 8
SECTIONS = 2
MOST = 64
N_ROW = 4
N_COL = 8


def block_flags(key, row_blocks, col_blocks, block_rows, block_cols, ceiling):
    number = row_blocks * col_blocks
    per_block = block_rows * block_cols
    first, second, third = jax.random.split(key, 3)
    counts = jax.random.randint(first, (number,), max(1, ceiling // 4), ceiling + 1)
    chosen = jax.random.randint(second, (), 0, number)
    counts = jnp.where(jnp.arange(number) == chosen, ceiling, counts)
    scores = jax.random.randint(third, (number, per_block), 0, 1 << 20) * per_block + jnp.arange(per_block)[None, :]
    order = jnp.argsort(scores, axis=1, stable=True)
    ranking = jnp.argsort(order, axis=1, stable=True)
    flags = (ranking < counts[:, None]).astype(jnp.int32)
    flags = flags.reshape(row_blocks, col_blocks, block_rows, block_cols).transpose(0, 2, 1, 3)
    return flags.reshape(row_blocks * block_rows, col_blocks * block_cols)


def draw_a_flags(key, part):
    return block_flags(jax.random.fold_in(key, 11), N_ROW, N_COL, TM_DEV, KT, MOST)


def draw_b_flags(key, part):
    return block_flags(jax.random.fold_in(key, 23), N_COL, N_COL, KT, TN_DEV, MOST)


def steps_of(own_key, shape, cuts, smallest, largest):
    factor_of, own = 1.0, jax.random.fold_in(own_key, 6)
    for dim, shards_of in cuts:
        heights = jnp.exp(jax.random.uniform(jax.random.fold_in(own, dim), (shards_of,), jnp.float32, smallest / len(cuts), largest / len(cuts)))
        factor_of = factor_of * jnp.repeat(heights, shape[dim] // shards_of).reshape([-1 if axis == dim else 1 for axis in range(len(shape))])
    return factor_of


def centred(own_key, shape, width, limit, cuts=(), held_as=jnp.bfloat16):
    drawn = width * jax.random.normal(own_key, shape, jnp.float32)
    if cuts:
        drawn = drawn * steps_of(own_key, shape, cuts, -0.22, 0.18)
    return jnp.clip(drawn, -limit, limit).astype(held_as)


def setup_inputs(seed: int = 0) -> dict:
    keys = jax.random.split(jax.random.key(seed), 6)
    a_matrix = centred(keys[0], (TILE * TM_DEV * N_ROW, TILE * KT * N_COL), 1.0, 6.0, ((0, 4), (1, 8)))
    a_flags = draw_a_flags(jax.random.fold_in(keys[5], 71), 0)
    b_matrix = centred(keys[2], (TILE * KT * N_COL, TILE * TN_DEV * N_COL), (KT * TILE) ** -0.5, 0.1875, ((0, 4), (1, 8)))
    b_flags = draw_b_flags(jax.random.fold_in(keys[5], 71), 0)
    sections = jax.random.randint(keys[4], (SECTIONS,), 0, N_COL).astype(jnp.int32)
    return {"a_matrix": a_matrix, "a_flags": a_flags, "b_matrix": b_matrix, "b_flags": b_flags, "sections": sections}


def mask_tiles(matrix, flags, tile_rows, tile_cols):
    shaped = matrix.reshape(tile_rows, TILE, tile_cols, TILE)
    shaped = shaped * flags.astype(matrix.dtype)[:, None, :, None]
    return shaped.reshape(tile_rows * TILE, tile_cols * TILE)


def to_tiles(matrix, tile_rows, tile_cols):
    return matrix.reshape(tile_rows, TILE, tile_cols, TILE).transpose(0, 2, 1, 3).reshape(tile_rows * tile_cols, TILE, TILE)


def from_tiles(tiles, tile_rows, tile_cols):
    return tiles.reshape(tile_rows, tile_cols, TILE, TILE).transpose(0, 2, 1, 3).reshape(tile_rows * TILE, tile_cols * TILE)


def compact(tiles, flags_flat, capacity):
    rank_of = jnp.cumsum(flags_flat) - 1
    slot_ids = jnp.arange(capacity, dtype=jnp.int32)
    matched = (flags_flat[None, :] == 1) & (rank_of[None, :] == slot_ids[:, None])
    source = jnp.sum(jnp.where(matched, jnp.arange(flags_flat.shape[0], dtype=jnp.int32)[None, :], 0), axis=1).astype(jnp.int32)
    is_valid = jnp.any(matched, axis=1)
    return jnp.take(tiles, source, axis=0) * is_valid.astype(tiles.dtype)[:, None, None]


def reference(a_matrix, a_flags, b_matrix, b_flags, sections):
    panel_width = KT * TILE

    def one_block(block):
        row_index = (block // N_COL).astype(jnp.int32)
        col_index = (block % N_COL).astype(jnp.int32)
        product = jnp.zeros((TM_DEV * TILE, TN_DEV * TILE), jnp.float32)
        intersection = jnp.zeros((TM_DEV, TN_DEV), jnp.float32)
        for step_index in range(SECTIONS):
            section = sections[step_index].astype(jnp.int32)
            a_panel = lax.dynamic_slice(a_matrix, (row_index * TM_DEV * TILE, section * panel_width), (TM_DEV * TILE, panel_width))
            a_panel_flags = lax.dynamic_slice(a_flags, (row_index * TM_DEV, section * KT), (TM_DEV, KT))
            b_panel = lax.dynamic_slice(b_matrix, (section * panel_width, col_index * TN_DEV * TILE), (panel_width, TN_DEV * TILE))
            b_panel_flags = lax.dynamic_slice(b_flags, (section * KT, col_index * TN_DEV), (KT, TN_DEV))
            a_masked = mask_tiles(a_panel, a_panel_flags, TM_DEV, KT)
            b_masked = mask_tiles(b_panel, b_panel_flags, KT, TN_DEV)
            product = product + jnp.dot(a_masked.astype(jnp.float32), b_masked.astype(jnp.float32), precision=lax.Precision.HIGHEST)
            intersection = intersection + jnp.dot(a_panel_flags.astype(jnp.float32), b_panel_flags.astype(jnp.float32), precision=lax.Precision.HIGHEST)
        occupied = (intersection > 0.5).astype(jnp.int32).reshape(-1)
        tiles = to_tiles(product.astype(jnp.bfloat16), TM_DEV, TN_DEV)
        packed_block = from_tiles(compact(tiles, occupied, TM_DEV * TN_DEV), TM_DEV, TN_DEV)
        return packed_block, jnp.sum(occupied).astype(jnp.int32)

    blocks, filled = lax.map(one_block, jnp.arange(N_ROW * N_COL, dtype=jnp.int32))
    offset = (jnp.cumsum(filled) - filled).astype(jnp.int32)
    slot_ids = jnp.arange(TM_DEV * TN_DEV, dtype=jnp.int32)
    places = jnp.where(slot_ids[None, :] < filled[:, None], offset[:, None] + slot_ids[None, :], -1).astype(jnp.int32)
    tile_place = places.reshape(N_ROW, N_COL, TM_DEV, TN_DEV).transpose(0, 2, 1, 3).reshape(N_ROW * TM_DEV, N_COL * TN_DEV)
    packed = blocks.reshape(N_ROW, N_COL, TM_DEV * TILE, TN_DEV * TILE).transpose(0, 2, 1, 3).reshape(N_ROW * TM_DEV * TILE, N_COL * TN_DEV * TILE)
    return packed, tile_place
```

```python
import functools

import jax
import jax.numpy as jnp
from jax import lax
from jax.experimental import pallas as pl
from jax.experimental.pallas import tpu as pltpu
from jax.sharding import PartitionSpec as P

TILE = 128
SECTIONS = 2
MOST = 64
CHUNKS = 8
VMEM = 56 * 1024 * 1024


def tile_at(index):
    return pl.ds(pl.multiple_of(index * TILE, TILE), TILE)


def pack_body(meta, flags, matrix, out, *, tile_rows, tile_cols):
    def clear(slot, carry):
        out[slot] = jnp.zeros((TILE, TILE), out.dtype)
        return carry

    lax.fori_loop(0, MOST, clear, 0)

    @pl.when(meta[0] == 1)
    def _():
        def lap(row, count):
            for col in range(tile_cols):
                flag = flags[row * tile_cols + col]
                slot = count

                @pl.when(flag == 1)
                def _():
                    out[slot] = matrix[tile_at(row), col * TILE : (col + 1) * TILE]

                count = count + flag
            return count

        lax.fori_loop(0, tile_rows, lap, jnp.int32(0))


def pack(matrix, flags, owner, block, tile_rows, tile_cols, name):
    meta = jnp.stack([owner.astype(jnp.int32), block.astype(jnp.int32)])
    return pl.pallas_call(
        functools.partial(pack_body, tile_rows=tile_rows, tile_cols=tile_cols),
        out_shape=jax.ShapeDtypeStruct((MOST, TILE, TILE), matrix.dtype),
        grid_spec=pltpu.PrefetchScalarGridSpec(
            num_scalar_prefetch=2,
            grid=(1,),
            in_specs=[
                pl.BlockSpec(
                    (tile_rows * TILE, tile_cols * TILE), lambda i, meta, flags: (meta[1], 0)
                )
            ],
            out_specs=pl.BlockSpec((MOST, TILE, TILE), lambda i, meta, flags: (0, 0, 0)),
        ),
        compiler_params=pltpu.CompilerParams(vmem_limit_bytes=VMEM),
        name=name,
    )(meta, flags.reshape(-1), matrix)


def expand_into(dense, flags, packed, tile_rows, tile_cols):
    def lap(row, count):
        for col in range(tile_cols):
            flag = flags[row * tile_cols + col]
            slot = count

            @pl.when(flag == 1)
            def _():
                dense[tile_at(row), col * TILE : (col + 1) * TILE] = packed[slot]

            @pl.when(flag != 1)
            def _():
                dense[tile_at(row), col * TILE : (col + 1) * TILE] = jnp.zeros(
                    (TILE, TILE), dense.dtype
                )

            count = count + flag
        return count

    lax.fori_loop(0, tile_rows, lap, jnp.int32(0))


def product_body(
    side, a_flags, b_flags, occupied, *refs, tile_rows, panel_tiles, tile_cols, step_tiles, chunk_tiles, last
):
    if last:
        mine0, mine1, other0, other1, b_packed, earlier, out, a_dense, b_dense, stage, rank = refs
    else:
        mine0, mine1, other0, other1, b_packed, out, a_dense, b_dense, stage = refs
    step = pl.program_id(0)
    piece = mine0.shape[1]

    @pl.when(step == 0)
    def _():
        for half in range(2):

            @pl.when(side[0] == half)
            def _():
                def move(slot, carry):
                    low, high = half * 2 * piece, (1 - half) * 2 * piece
                    stage[low + slot] = mine0[0, slot]
                    stage[low + piece + slot] = mine1[0, slot]
                    stage[high + slot] = other0[0, slot]
                    stage[high + piece + slot] = other1[0, slot]
                    return carry

                lax.fori_loop(0, piece, move, 0)

        expand_into(a_dense, a_flags, stage, tile_rows, panel_tiles)
        expand_into(b_dense, b_flags, b_packed, panel_tiles, tile_cols)
        if last:

            def lap(tile, count):
                rank[tile] = count
                return count + occupied[tile]

            filled = lax.fori_loop(0, tile_rows * tile_cols, lap, jnp.int32(0))

            def clear(slot, carry):
                out[tile_at(slot // tile_cols), tile_at(slot % tile_cols)] = jnp.zeros(
                    (TILE, TILE), out.dtype
                )
                return carry

            lax.fori_loop(filled, tile_rows * tile_cols, clear, 0)

    rows = step_tiles * TILE
    left = a_dense[pl.ds(pl.multiple_of(step * rows, rows), rows), :]
    for chunk in range(tile_cols // chunk_tiles):
        cols = slice(chunk * chunk_tiles * TILE, (chunk + 1) * chunk_tiles * TILE)
        part = jnp.dot(left, b_dense[:, cols], preferred_element_type=jnp.float32)
        if not last:
            out[:, cols] = part
            continue
        part = (part + earlier[:, cols]).astype(out.dtype)
        for row in range(step_tiles):
            for col in range(chunk_tiles):
                tile = (step * step_tiles + row) * tile_cols + chunk * chunk_tiles + col
                slot = rank[tile]

                @pl.when(occupied[tile] == 1)
                def _():
                    out[tile_at(slot // tile_cols), tile_at(slot % tile_cols)] = part[
                        row * TILE : (row + 1) * TILE, col * TILE : (col + 1) * TILE
                    ]


def product(section, side, a_flags, b_flags, occupied, pieces, b_packed, earlier):
    tile_rows, panel_tiles = a_flags.shape
    tile_cols = b_flags.shape[1]
    last = earlier is not None
    step_tiles, chunk_tiles = min(4, tile_rows), min(4, tile_cols)
    piece = pieces[0].shape[1]
    rows, cols, depth = tile_rows * TILE, tile_cols * TILE, panel_tiles * TILE
    strip = pl.BlockSpec((step_tiles * TILE, cols), lambda i, *_: (i, 0))
    in_specs = [
        pl.BlockSpec((1, piece, TILE, TILE), lambda i, *_: (section, 0, 0, 0)) for _ in pieces
    ] + [pl.BlockSpec((MOST, TILE, TILE), lambda i, *_: (0, 0, 0))]
    operands = [*pieces, b_packed]
    scratch = [
        pltpu.VMEM((rows, depth), jnp.bfloat16),
        pltpu.VMEM((depth, cols), jnp.bfloat16),
        pltpu.VMEM((MOST, TILE, TILE), jnp.bfloat16),
    ]
    if last:
        in_specs.append(strip)
        operands.append(earlier)
        scratch.append(pltpu.SMEM((tile_rows * tile_cols,), jnp.int32))
    return pl.pallas_call(
        functools.partial(
            product_body,
            tile_rows=tile_rows,
            panel_tiles=panel_tiles,
            tile_cols=tile_cols,
            step_tiles=step_tiles,
            chunk_tiles=chunk_tiles,
            last=last,
        ),
        out_shape=jax.ShapeDtypeStruct((rows, cols), jnp.bfloat16 if last else jnp.float32),
        grid_spec=pltpu.PrefetchScalarGridSpec(
            num_scalar_prefetch=4,
            grid=(tile_rows // step_tiles,),
            in_specs=in_specs,
            out_specs=pl.BlockSpec((rows, cols), lambda i, *_: (0, 0)) if last else strip,
            scratch_shapes=scratch,
        ),
        compiler_params=pltpu.CompilerParams(vmem_limit_bytes=VMEM),
        name="last_product" if last else "first_product",
    )(side.reshape(1), a_flags.reshape(-1), b_flags.reshape(-1), occupied.reshape(-1), *operands)


def swap(value, axis, bit):
    length = lax.axis_size(axis)
    return lax.ppermute(value, axis, [(i, i ^ (1 << bit)) for i in range(length)])


def spread_a(own, sections):
    position = lax.axis_index("col")
    top = lax.axis_size("col").bit_length() - 1
    side = position & 1
    halves = own.reshape(2, MOST // 2, TILE, TILE)
    keep = lax.dynamic_index_in_dim(halves, side, 0, keepdims=False)
    give = lax.dynamic_index_in_dim(halves, 1 - side, 0, keepdims=False)
    got = swap(give, "col", 0)
    piece = MOST // 4
    distance = jnp.bitwise_xor(position, sections)
    mask_of = lambda flags: flags[:, None, None, None]
    pieces = []
    for which in range(2):
        part = slice(which * piece, (which + 1) * piece)
        held = jnp.where(mask_of((distance & 1) == 0), keep[None, part], got[None, part])
        order = list(range(1, top))
        shift = which % max(1, len(order))
        pieces.append([held, order[shift:] + order[:shift]])
    missing = [(1 << top) - 2, (1 << top) - 2]
    for lap in range(top - 1):
        for which in range(2):
            held, order = pieces[which]
            bit = order[lap]
            arrived = swap(held, "col", bit)
            has = (distance & missing[which]) == 0
            pieces[which][0] = jnp.where(mask_of(has), held, arrived)
            missing[which] &= ~(1 << bit)
    mine = [held for held, _ in pieces]
    return side, mine + [swap(held, "col", 0) for held in mine]


def spread_b(own, owner):
    position, length = lax.axis_index("row"), lax.axis_size("row")
    up = [(i, i + 1) for i in range(length - 1)]
    down = [(i + 1, i) for i in range(length - 1)]
    chunk = MOST // CHUNKS
    is_owner = position == owner
    sent = own[:chunk]
    arrived = []
    for step in range(CHUNKS + length - 2):
        below, above = lax.ppermute(sent, "row", up), lax.ppermute(sent, "row", down)
        got = jnp.where(position > owner, below, above)
        arrived.append(got)
        start = min(step + 1, CHUNKS - 1) * chunk
        sent = jnp.where(is_owner, own[start : start + chunk], got)
    first = (jnp.maximum(jnp.abs(position - owner), 1) - 1) * chunk
    panel = lax.dynamic_slice_in_dim(jnp.concatenate(arrived), first, MOST, 0)
    return jnp.where(is_owner, own, panel)


def shards(a_matrix, a_flags, b_matrix, b_flags, sections):
    tile_rows, panel_tiles = a_flags.shape
    b_tiles, tile_cols = b_flags.shape
    n_row, n_col = lax.axis_size("row"), lax.axis_size("col")
    my_row, my_col = lax.axis_index("row"), lax.axis_index("col")
    ratio = n_col // n_row
    owner_row = sections // ratio
    block = sections % ratio
    b_got = []
    for step in range(SECTIONS):
        own_flags = lax.dynamic_slice_in_dim(b_flags, block[step] * panel_tiles, panel_tiles, 0)
        b_send = pack(
            b_matrix, own_flags, owner_row[step] == my_row, block[step], panel_tiles, tile_cols, "pack_b"
        )
        b_got.append(spread_b(b_send, owner_row[step]))
    one = jnp.int32(1)
    a_own = pack(a_matrix, a_flags, one, one * 0, tile_rows, panel_tiles, "pack_a")
    side, pieces = spread_a(a_own, sections)

    flags = jnp.concatenate([a_flags.reshape(-1), b_flags.reshape(-1)])
    every = lax.all_gather(flags, ("row", "col"))
    a_every = every[:, : a_flags.size].reshape(n_row, n_col, tile_rows, panel_tiles)
    b_every = every[:, a_flags.size :].reshape(n_row, n_col, b_tiles, tile_cols)
    meet = jnp.zeros((n_row, tile_rows, n_col, tile_cols), jnp.float32)
    a_mine, b_mine = [], []
    for step in range(SECTIONS):
        a_part = lax.dynamic_index_in_dim(a_every, sections[step], 1, keepdims=False)
        b_part = lax.dynamic_index_in_dim(b_every, owner_row[step], 0, keepdims=False)
        b_part = lax.dynamic_slice_in_dim(b_part, block[step] * panel_tiles, panel_tiles, 1)
        meet = meet + jnp.einsum(
            "rik,ckj->ricj",
            a_part.astype(jnp.float32),
            b_part.astype(jnp.float32),
            precision=lax.Precision.HIGHEST,
        )
        a_mine.append(lax.dynamic_index_in_dim(a_part, my_row, 0, keepdims=False))
        b_mine.append(lax.dynamic_index_in_dim(b_part, my_col, 0, keepdims=False))
    occupied_all = (meet > 0.5).astype(jnp.int32)
    filled = jnp.sum(occupied_all, axis=(1, 3)).reshape(-1)
    number = my_row * n_col + my_col
    numbers = jnp.arange(n_row * n_col, dtype=jnp.int32)
    offset = jnp.sum(jnp.where(numbers < number, filled, 0))
    own_filled = jnp.sum(jnp.where(numbers == number, filled, 0))
    slots = jnp.arange(tile_rows * tile_cols, dtype=jnp.int32).reshape(tile_rows, tile_cols)
    places = jnp.where(slots < own_filled, offset + slots, -1).astype(jnp.int32)
    occupied = lax.dynamic_slice(
        occupied_all, (my_row, 0, my_col, 0), (1, tile_rows, 1, tile_cols)
    ).reshape(tile_rows, tile_cols)

    total = None
    for step in range(SECTIONS):
        total = product(
            step, side, a_mine[step], b_mine[step], occupied, pieces, b_got[step], total
        )
    return total, places


def solution(mesh):
    return jax.shard_map(
        shards,
        mesh=mesh,
        in_specs=(P("row", "col"), P("row", "col"), P("row", "col"), P("row", "col"), P()),
        out_specs=(P("row", "col"), P("row", "col")),
        check_vma=False,
    )
```
